32 devices in a mesh: rep: 16 (over z, x, core), tp: 2 (over y).
Axes of the slice: x: 2, y: 2, z: 4, core: 2. Of those that a mesh axis runs over, the one named last changes fastest.
Arguments:
- tokens: bfloat16 [16, 256, 3072], P('rep', 'tp'), may hold values from -100 to 100
- norm_gain: float32 [16, 3072], P('rep'), may hold values from 0.5 to 1.5
- w_query: bfloat16 [16, 3072, 2048], P('rep', None, 'tp'), may hold values from -1 to 1
- key_weight: bfloat16 [16, 3072, 1024], P('rep', None, 'tp'), may hold values from -1 to 1
- value_weight: bfloat16 [16, 3072, 1024], P('rep', None, 'tp'), may hold values from -0.109375 to 0.109375
- attention_gradient: bfloat16 [16, 256, 2048], P('rep', None, 'tp'), may hold values from -6 to 6
- global_fragment: float32 [128, 3072], P('tp'), may hold values from -6 to 6
- momentum: float32 [128, 3072], P('tp'), may hold values from -3 to 3
- local_fragment: bfloat16 [16, 128, 3072], P('rep', 'tp'), may hold values from -6 to 6
Outputs:
- grad_query_w: bfloat16 [16, 3072, 2048], P('rep', None, 'tp')
- grad_key_w: bfloat16 [16, 3072, 1024], P('rep', None, 'tp')
- grad_value_w: bfloat16 [16, 3072, 1024], P('rep', None, 'tp')
- grad_gain: float32 [16, 3072], P('rep')
- grad_tokens: bfloat16 [16, 256, 3072], P('rep', 'tp')
- new_global: float32 [128, 3072], P('tp')
- new_momentum: float32 [128, 3072], P('tp')
The draws below stay inside these ranges and needn't reach their ends.
All inputs are finite; a program needn't handle non-finite values.
Results may differ from the reference program's by a relative error of at most 0.019.
The reference program's roundings to bfloat16 on the way count: a program that leaves them out, or rounds other values in their place, can miss the bound.
Values may be sent and summed in bfloat16 or wider, within the bound.
A program may use at most 128 MiB of HBM per device.

```python
import math
import jax
import jax.numpy as jnp
from jax import lax

MODEL_WIDTH = 3072
QUERY_HEADS = 16
KEY_VALUE_HEADS = 8
HEAD_SIZE = 128
SEQ = 256
FRAG = 128
N_REP = 16
N_TP = 2


def draw_tokens(key, part):
    col_scale = jnp.exp(jax.random.uniform(jax.random.fold_in(key, 12), (1, 1, MODEL_WIDTH), jnp.float32, math.log(0.5), math.log(2.0)))
    row_scale = jnp.exp(jax.random.uniform(jax.random.fold_in(key, 11), (N_REP, SEQ, 1), jnp.float32, 0.0, math.log(10.0)))
    jitter = jax.random.normal(jax.random.fold_in(key, 13), (N_REP, SEQ, MODEL_WIDTH), jnp.float32)
    result = jitter * col_scale * row_scale
    return jnp.clip(result, -100.0, 100.0).astype(jnp.bfloat16)


def draw_w_query(key, part):
    return (jax.random.normal(jax.random.fold_in(key, 21), (N_REP, MODEL_WIDTH, QUERY_HEADS * HEAD_SIZE), jnp.float32) * MODEL_WIDTH ** (-0.5)).astype(jnp.bfloat16)


def draw_key_weight(key, part):
    return (jax.random.normal(jax.random.fold_in(key, 31), (N_REP, MODEL_WIDTH, KEY_VALUE_HEADS * HEAD_SIZE), jnp.float32) * MODEL_WIDTH ** (-0.5)).astype(jnp.bfloat16)


def levels(own_key, shape, pieces, low, largest):
    level, own = 1.0, jax.random.fold_in(own_key, 6)
    for dim, parts in pieces:
        heights = jnp.exp(jax.random.uniform(jax.random.fold_in(own, dim), (parts,), jnp.float32, low / len(pieces), largest / len(pieces)))
        level = level * jnp.repeat(heights, shape[dim] // parts).reshape([-1 if axis == dim else 1 for axis in range(len(shape))])
    return level


def centred(own_key, shape, spread, reach, cuts=(), kind=jnp.bfloat16):
    array = jax.random.normal(own_key, shape, jnp.float32) * spread
    if len(cuts) > 0:
        array = levels(own_key, shape, cuts, -0.22, 0.18) * array
    return jnp.clip(array, min=-reach, max=reach).astype(kind)


def setup_inputs(seed: int = 0) -> dict:
    seeds = jax.random.split(jax.random.key(seed), 10)
    return {
        "tokens": draw_tokens(jax.random.fold_in(seeds[9], 71), 0),
        "norm_gain": jnp.clip(1.0 + 0.1 * jax.random.normal(seeds[1], (N_REP, MODEL_WIDTH), jnp.float32), 0.5, 1.5),
        "w_query": draw_w_query(jax.random.fold_in(seeds[9], 71), 0),
        "key_weight": draw_key_weight(jax.random.fold_in(seeds[9], 71), 0),
        "value_weight": centred(seeds[4], (N_REP, MODEL_WIDTH, KEY_VALUE_HEADS * HEAD_SIZE), MODEL_WIDTH ** -0.5, 0.109375, ((0, 16), (2, 2))),
        "attention_gradient": centred(seeds[5], (N_REP, SEQ, QUERY_HEADS * HEAD_SIZE), 1.0, 6.0, ((0, 16), (2, 2))),
        "global_fragment": centred(seeds[6], (FRAG, MODEL_WIDTH), 1.0, 6.0, ((0, 2),), jnp.float32),
        "momentum": centred(seeds[7], (FRAG, MODEL_WIDTH), 0.5, 3.0, ((0, 2),), jnp.float32),
        "local_fragment": centred(seeds[8], (N_REP, FRAG, MODEL_WIDTH), 1.0, 6.0, ((0, 16), (1, 2))),
    }


epsilon = 1e-05
rope_base = 500000.0
outer_rate = 0.7
outer_momentum = 0.9

def rope_tables(sequence_length, width):
    middle = width // 2
    frequency = rope_base ** (-2.0 * jnp.arange(middle, dtype=jnp.float32) / width)
    angles = jnp.arange(sequence_length, dtype=jnp.float32)[:, None] * frequency[None, :]
    angles = jnp.concatenate([angles, angles], axis=1)
    return (jnp.cos(angles)[:, None, :], jnp.sin(angles)[:, None, :])

def rotate(vectors, cosine_table, sine_table):
    middle = vectors.shape[-1] // 2
    turned = jnp.concatenate([-vectors[..., middle:], vectors[..., :middle]], axis=-1)
    return vectors * cosine_table + turned * sine_table

def reverse_rotation(gradient, cosine_table, sine_table):
    middle = gradient.shape[-1] // 2
    shifted = gradient * sine_table
    turned = jnp.concatenate([shifted[..., middle:], -shifted[..., :middle]], axis=-1)
    return gradient * cosine_table + turned

def attention_reverse(query_rows, rotated_keys, values_bfloat, grad_out, block_of_rows):
    sequence_length = query_rows.shape[0]
    score_scale = query_rows.shape[-1] ** (-0.5)
    keys_wide = rotated_keys.astype(jnp.float32)
    values_wide = values_bfloat.astype(jnp.float32)

    def one_block(running, block_index):
        acc_key, acc_value = running
        offset = block_index * block_of_rows
        query_block = lax.dynamic_slice_in_dim(query_rows, offset, block_of_rows, 0).astype(jnp.float32)
        grad_block = lax.dynamic_slice_in_dim(grad_out, offset, block_of_rows, 0).astype(jnp.float32)
        scores = jnp.einsum('qgrd,kgd->grqk', query_block, keys_wide) * score_scale
        row_pos = offset + jnp.arange(block_of_rows)
        col_pos = jnp.arange(sequence_length)
        allowed = col_pos[None, :] <= row_pos[:, None]
        scores = jnp.where(allowed, scores, -jnp.inf)
        highest = lax.optimization_barrier(jnp.max(scores, axis=-1, keepdims=True))
        powers = jnp.exp(scores - highest)
        probability = powers / lax.optimization_barrier(jnp.sum(powers, axis=-1, keepdims=True))
        prob_low = lax.optimization_barrier(probability.astype(jnp.bfloat16)).astype(jnp.float32)
        acc_value = acc_value + jnp.einsum('grqk,qgrd->kgd', prob_low, grad_block)
        grad_prob = jnp.einsum('qgrd,kgd->grqk', grad_block, values_wide)
        grad_score = probability * (grad_prob - lax.optimization_barrier(jnp.sum(grad_prob * probability, axis=-1, keepdims=True))) * score_scale
        score_low = lax.optimization_barrier(grad_score.astype(jnp.bfloat16)).astype(jnp.float32)
        grad_query = jnp.einsum('grqk,kgd->qgrd', score_low, keys_wide)
        acc_key = acc_key + jnp.einsum('grqk,qgrd->kgd', score_low, query_block)
        return ((acc_key, acc_value), grad_query)
    initial = jnp.zeros(rotated_keys.shape, jnp.float32)
    (acc_key, acc_value), grad_blocks = lax.scan(one_block, (initial, initial), jnp.arange(sequence_length // block_of_rows))
    grad_query = grad_blocks.reshape(query_rows.shape)
    return (grad_query, acc_key, acc_value)

def replica_grads(items):
    tokens, norm_gains, w_query, key_weight, value_weight, attention_gradient = items
    sequence_length = tokens.shape[0]
    widened_rows = tokens.astype(jnp.float32)
    inverse_norm = lax.rsqrt(lax.optimization_barrier(jnp.mean(widened_rows * widened_rows, axis=-1, keepdims=True)) + epsilon)
    normalized_input = widened_rows * inverse_norm
    normalized = (normalized_input * norm_gains[None, :]).astype(jnp.bfloat16)
    cosine_table, sine_table = rope_tables(sequence_length, HEAD_SIZE)
    query_rows = jnp.dot(normalized, w_query, preferred_element_type=jnp.float32).reshape(sequence_length, QUERY_HEADS, HEAD_SIZE)
    query_rows = rotate(query_rows, cosine_table, sine_table).astype(jnp.bfloat16)
    rotated_keys = jnp.dot(normalized, key_weight, preferred_element_type=jnp.float32).reshape(sequence_length, KEY_VALUE_HEADS, HEAD_SIZE)
    rotated_keys = rotate(rotated_keys, cosine_table, sine_table).astype(jnp.bfloat16)
    values_bfloat = jnp.dot(normalized, value_weight, preferred_element_type=jnp.float32).astype(jnp.bfloat16).reshape(sequence_length, KEY_VALUE_HEADS, HEAD_SIZE)
    replica_group = QUERY_HEADS // KEY_VALUE_HEADS
    block_of_rows = min(512, sequence_length)
    query_input_gradient, key_input_gradient, value_input_gradient = attention_reverse(query_rows.reshape(sequence_length, KEY_VALUE_HEADS, replica_group, HEAD_SIZE), rotated_keys, values_bfloat, attention_gradient.reshape(sequence_length, KEY_VALUE_HEADS, replica_group, HEAD_SIZE), block_of_rows)
    dquery = reverse_rotation(query_input_gradient.reshape(sequence_length, QUERY_HEADS, HEAD_SIZE), cosine_table, sine_table).astype(jnp.bfloat16).reshape(sequence_length, QUERY_HEADS * HEAD_SIZE)
    key_gradient = reverse_rotation(key_input_gradient, cosine_table, sine_table).astype(jnp.bfloat16).reshape(sequence_length, KEY_VALUE_HEADS * HEAD_SIZE)
    value_gradient = value_input_gradient.astype(jnp.bfloat16).reshape(sequence_length, KEY_VALUE_HEADS * HEAD_SIZE)
    contract = (((0,), (0,)), ((), ()))
    grad_wq = lax.dot_general(normalized, dquery, contract, preferred_element_type=jnp.float32).astype(jnp.bfloat16)
    grad_wk = lax.dot_general(normalized, key_gradient, contract, preferred_element_type=jnp.float32).astype(jnp.bfloat16)
    grad_wv = lax.dot_general(normalized, value_gradient, contract, preferred_element_type=jnp.float32).astype(jnp.bfloat16)
    query_cols = QUERY_HEADS * HEAD_SIZE // N_TP
    key_value_columns = KEY_VALUE_HEADS * HEAD_SIZE // N_TP
    back = (((1,), (1,)), ((), ()))
    summed_rows = jnp.zeros((sequence_length, MODEL_WIDTH), jnp.float32)
    for shard_index in range(N_TP):
        qa, qb_end = (shard_index * query_cols, (shard_index + 1) * query_cols)
        ka, kb_end = (shard_index * key_value_columns, (shard_index + 1) * key_value_columns)
        partial_value = lax.dot_general(dquery[:, qa:qb_end], w_query[:, qa:qb_end], back, preferred_element_type=jnp.float32)
        partial_value = partial_value + lax.dot_general(key_gradient[:, ka:kb_end], key_weight[:, ka:kb_end], back, preferred_element_type=jnp.float32)
        partial_value = partial_value + lax.dot_general(value_gradient[:, ka:kb_end], value_weight[:, ka:kb_end], back, preferred_element_type=jnp.float32)
        summed_rows = summed_rows + lax.optimization_barrier(partial_value.astype(jnp.bfloat16)).astype(jnp.float32)
    gains_gradient = lax.optimization_barrier(jnp.sum(summed_rows * normalized_input, axis=0))
    scaled_rows = summed_rows * norm_gains[None, :]
    gradient_rows = inverse_norm * (scaled_rows - normalized_input * lax.optimization_barrier(jnp.mean(scaled_rows * normalized_input, axis=-1, keepdims=True)))
    return (grad_wq, grad_wk, grad_wv, gains_gradient, gradient_rows.astype(jnp.bfloat16))

def reference(tokens, norm_gain, w_query, key_weight, value_weight, attention_gradient, global_fragment, momentum, local_fragment):
    grad_wq, grad_wk, grad_wv, gains_gradient, gradient_rows = lax.map(replica_grads, (tokens, norm_gain, w_query, key_weight, value_weight, attention_gradient))
    delta = global_fragment[None, :, :] - local_fragment.astype(jnp.float32)
    mean_delta = lax.optimization_barrier(jnp.sum(delta, axis=0)) / N_REP
    new_momentum = outer_momentum * momentum + mean_delta
    new_global = global_fragment - outer_rate * (mean_delta + outer_momentum * new_momentum)
    return (grad_wq, grad_wk, grad_wv, gains_gradient, gradient_rows, new_global, new_momentum)
```

```python
import functools

import jax
import jax.numpy as jnp
import numpy as np
from jax import lax
from jax.experimental import pallas as pl
from jax.experimental.pallas import tpu as pltpu
from jax.sharding import PartitionSpec as P

MESH = pl.DeviceIdType.MESH

HEAD_SIZE = 128


epsilon = 1e-05
rope_base = 500000.0
outer_rate = 0.7
outer_momentum = 0.9


def rope_tables(sequence_length, width):
    middle = width // 2
    frequency = rope_base ** (-2.0 * jnp.arange(middle, dtype=jnp.float32) / width)
    angles = jnp.arange(sequence_length, dtype=jnp.float32)[:, None] * frequency[None, :]
    angles = jnp.concatenate([angles, angles], axis=1)
    return (jnp.cos(angles)[:, None, :], jnp.sin(angles)[:, None, :])


def rotate(vectors, cosine_table, sine_table):
    middle = vectors.shape[-1] // 2
    turned = jnp.concatenate([-vectors[..., middle:], vectors[..., :middle]], axis=-1)
    return vectors * cosine_table + turned * sine_table


def reverse_rotation(gradient, cosine_table, sine_table):
    middle = gradient.shape[-1] // 2
    shifted = gradient * sine_table
    turned = jnp.concatenate([shifted[..., middle:], -shifted[..., :middle]], axis=-1)
    return gradient * cosine_table + turned


def attention_reverse(query_rows, rotated_keys, values_bfloat, grad_out, block_of_rows):
    sequence_length = query_rows.shape[0]
    score_scale = query_rows.shape[-1] ** (-0.5)

    def one_block(running, block_index):
        acc_key, acc_value = running
        offset = block_index * block_of_rows
        query_block = lax.dynamic_slice_in_dim(query_rows, offset, block_of_rows, 0)
        grad_block = lax.dynamic_slice_in_dim(grad_out, offset, block_of_rows, 0)
        scores = (
            jnp.einsum(
                "qgrd,kgd->grqk", query_block, rotated_keys, preferred_element_type=jnp.float32
            )
            * score_scale
        )
        row_pos = offset + jnp.arange(block_of_rows)
        col_pos = jnp.arange(sequence_length)
        allowed = col_pos[None, :] <= row_pos[:, None]
        scores = jnp.where(allowed, scores, -jnp.inf)
        highest = jnp.max(scores, axis=-1, keepdims=True)
        powers = jnp.exp(scores - highest)
        probability = powers / jnp.sum(powers, axis=-1, keepdims=True)
        prob_low = probability.astype(jnp.bfloat16)
        acc_value = acc_value + jnp.einsum(
            "grqk,qgrd->kgd", prob_low, grad_block, preferred_element_type=jnp.float32
        )
        grad_prob = jnp.einsum(
            "qgrd,kgd->grqk", grad_block, values_bfloat, preferred_element_type=jnp.float32
        )
        grad_score = (
            probability
            * (grad_prob - jnp.sum(grad_prob * probability, axis=-1, keepdims=True))
            * score_scale
        )
        score_low = grad_score.astype(jnp.bfloat16)
        grad_query = jnp.einsum(
            "grqk,kgd->qgrd", score_low, rotated_keys, preferred_element_type=jnp.float32
        )
        acc_key = acc_key + jnp.einsum(
            "grqk,qgrd->kgd", score_low, query_block, preferred_element_type=jnp.float32
        )
        return ((acc_key, acc_value), grad_query)

    initial = jnp.zeros(rotated_keys.shape, jnp.float32)
    (acc_key, acc_value), grad_blocks = lax.scan(
        one_block, (initial, initial), jnp.arange(sequence_length // block_of_rows)
    )
    return (grad_blocks.reshape(query_rows.shape), acc_key, acc_value)


def body(
    tokens,
    norm_gain,
    w_query,
    key_weight,
    value_weight,
    attention_gradient,
    global_fragment,
    momentum,
    local_fragment,
):
    local_rows = tokens[0]
    norm_gains = norm_gain[0]
    weight_q = w_query[0]
    weight_k = key_weight[0]
    weight_v = value_weight[0]
    widened_rows = local_rows.astype(jnp.float32)
    inverse_norm = lax.rsqrt(
        jnp.mean(widened_rows * widened_rows, axis=-1, keepdims=True) + epsilon
    )
    normalized_input = widened_rows * inverse_norm
    normalized_local = (normalized_input * norm_gains[None, :]).astype(jnp.bfloat16)
    normalized = lax.all_gather(normalized_local, "tp", axis=0, tiled=True)
    sequence_length = normalized.shape[0]
    heads_q = weight_q.shape[1] // HEAD_SIZE
    heads_kv = weight_k.shape[1] // HEAD_SIZE
    cosine_table, sine_table = rope_tables(sequence_length, HEAD_SIZE)
    query_rows = jnp.dot(normalized, weight_q, preferred_element_type=jnp.float32).reshape(
        sequence_length, heads_q, HEAD_SIZE
    )
    query_rows = rotate(query_rows, cosine_table, sine_table).astype(jnp.bfloat16)
    rotated_keys = jnp.dot(normalized, weight_k, preferred_element_type=jnp.float32).reshape(
        sequence_length, heads_kv, HEAD_SIZE
    )
    rotated_keys = rotate(rotated_keys, cosine_table, sine_table).astype(jnp.bfloat16)
    values_bfloat = (
        jnp.dot(normalized, weight_v, preferred_element_type=jnp.float32)
        .astype(jnp.bfloat16)
        .reshape(sequence_length, heads_kv, HEAD_SIZE)
    )
    replica_group = heads_q // heads_kv
    block_of_rows = min(512, sequence_length)
    query_input_gradient, key_input_gradient, value_input_gradient = attention_reverse(
        query_rows.reshape(sequence_length, heads_kv, replica_group, HEAD_SIZE),
        rotated_keys,
        values_bfloat,
        attention_gradient[0].reshape(sequence_length, heads_kv, replica_group, HEAD_SIZE),
        block_of_rows,
    )
    dquery = (
        reverse_rotation(
            query_input_gradient.reshape(sequence_length, heads_q, HEAD_SIZE),
            cosine_table,
            sine_table,
        )
        .astype(jnp.bfloat16)
        .reshape(sequence_length, heads_q * HEAD_SIZE)
    )
    key_gradient = (
        reverse_rotation(key_input_gradient, cosine_table, sine_table)
        .astype(jnp.bfloat16)
        .reshape(sequence_length, heads_kv * HEAD_SIZE)
    )
    value_gradient = value_input_gradient.astype(jnp.bfloat16).reshape(
        sequence_length, heads_kv * HEAD_SIZE
    )
    contract = (((0,), (0,)), ((), ()))
    grad_wq = lax.dot_general(
        normalized, dquery, contract, preferred_element_type=jnp.float32
    ).astype(jnp.bfloat16)
    grad_wk = lax.dot_general(
        normalized, key_gradient, contract, preferred_element_type=jnp.float32
    ).astype(jnp.bfloat16)
    grad_wv = lax.dot_general(
        normalized, value_gradient, contract, preferred_element_type=jnp.float32
    ).astype(jnp.bfloat16)
    back = (((1,), (1,)), ((), ()))
    partial_value = lax.dot_general(dquery, weight_q, back, preferred_element_type=jnp.float32)
    partial_value = partial_value + lax.dot_general(
        key_gradient, weight_k, back, preferred_element_type=jnp.float32
    )
    summed_rows = lax.psum_scatter(
        (
            partial_value
            + lax.dot_general(value_gradient, weight_v, back, preferred_element_type=jnp.float32)
        ).astype(jnp.bfloat16),
        "tp",
        scatter_dimension=0,
        tiled=True,
    ).astype(jnp.float32)
    gains_gradient = lax.psum(jnp.sum(summed_rows * normalized_input, axis=0), "tp")
    scaled_rows = summed_rows * norm_gains[None, :]
    gradient_rows = (
        inverse_norm
        * (
            scaled_rows
            - normalized_input * jnp.mean(scaled_rows * normalized_input, axis=-1, keepdims=True)
        )
    ).astype(jnp.bfloat16)
    delta = global_fragment - local_fragment[0].astype(jnp.float32)
    replicas = lax.axis_size("rep")
    mean_delta = lax.psum(delta, "rep") / replicas
    new_momentum = outer_momentum * momentum + mean_delta
    new_global = global_fragment - outer_rate * (mean_delta + outer_momentum * new_momentum)
    return (
        grad_wq[None],
        grad_wk[None],
        grad_wv[None],
        gains_gradient[None],
        gradient_rows[None],
        new_global,
        new_momentum,
    )

NT = (((1,), (1,)), ((), ()))
TN = (((0,), (0,)), ((), ()))


def dot(a, b, dims=(((1,), (0,)), ((), ()))):
    return lax.dot_general(a, b, dims, preferred_element_type=jnp.float32)


def ds(index, size):
    return pl.ds(pl.multiple_of(index * size, size), size)


def host_tables(sequence_length, width):
    middle = width // 2
    frequency = rope_base ** (-2.0 * np.arange(middle) / width)
    angles = np.arange(sequence_length)[:, None] * frequency[None, :]
    cosine, sine = np.cos(angles), np.sin(angles)
    return (
        jnp.asarray(np.concatenate([cosine, cosine], axis=1), jnp.float32),
        jnp.asarray(np.concatenate([-sine, sine], axis=1), jnp.float32),
    )


def front_kernel(
    n_rep,
    chunks,
    tile,
    tokens_ref,
    gain_ref,
    wq_hbm,
    wk_hbm,
    wv_hbm,
    go_ref,
    cos_ref,
    sin_ref,
    local_hbm,
    normed_ref,
    dq_ref,
    dk_ref,
    dv_ref,
    mean_ref,
    w_ref,
    nm_ref,
    acc_ref,
    q_ref,
    k_ref,
    v_ref,
    pieces_ref,
    own_mean_ref,
    all_mean_ref,
    w_sems,
    ag_send,
    ag_recv,
    fr_send,
    fr_recv,
    fg_send,
    fg_recv,
    own_sem,
):
    me = lax.axis_index("tp")
    peer = 1 - me
    rep = lax.axis_index("rep")
    rows, width = tokens_ref.shape
    qw, kw = wq_hbm.shape[1], wk_hbm.shape[1]
    total = qw + 2 * kw
    cw = width // chunks
    piece_rows, piece_cols = own_mean_ref.shape
    col_blocks = width // piece_cols
    barrier = pltpu.get_barrier_semaphore()
    pl.semaphore_signal(barrier, inc=1, device_id={"tp": peer}, device_id_type=MESH)

    def greet(j, _):
        pl.semaphore_signal(
            barrier, inc=1, device_id={"rep": lax.rem(rep + j, n_rep)}, device_id_type=MESH
        )
        return 0

    lax.fori_loop(1, n_rep, greet, 0)
    weight_copies = [
        pltpu.make_async_copy(wq_hbm, w_ref.at[:, pl.ds(0, qw)], w_sems.at[0]),
        pltpu.make_async_copy(wk_hbm, w_ref.at[:, pl.ds(qw, kw)], w_sems.at[1]),
        pltpu.make_async_copy(wv_hbm, w_ref.at[:, pl.ds(qw + kw, kw)], w_sems.at[2]),
    ]
    for copy in weight_copies:
        copy.start()

    def piece(owner):
        return (
            ds(owner // col_blocks, piece_rows),
            ds(lax.rem(owner, col_blocks), piece_cols),
        )

    own_piece = pltpu.make_async_copy(local_hbm.at[piece(rep)], pieces_ref.at[0], own_sem)
    own_piece.start()

    step = 16

    def norm_rows(i, _):
        x = tokens_ref[ds(i, step), :].astype(jnp.float32)
        inverse = lax.rsqrt(jnp.mean(x * x, axis=-1, keepdims=True) + epsilon)
        nm_ref[pl.ds(pl.multiple_of(me * rows + i * step, step), step), :] = (
            x * inverse * gain_ref[...]
        ).astype(jnp.bfloat16)
        return 0

    lax.fori_loop(0, rows // step, norm_rows, 0)
    pl.semaphore_wait(barrier, n_rep)

    def gather_copy(c):
        part = nm_ref.at[ds(me, rows), ds(c, cw)]
        return pltpu.make_async_remote_copy(
            src_ref=part,
            dst_ref=part,
            send_sem=ag_send.at[c],
            recv_sem=ag_recv.at[c],
            device_id={"tp": peer},
            device_id_type=MESH,
        )

    def scatter_copy(j):
        target = lax.rem(rep + j, n_rep)
        return pltpu.make_async_remote_copy(
            src_ref=local_hbm.at[piece(target)],
            dst_ref=pieces_ref.at[j],
            send_sem=fr_send.at[j],
            recv_sem=fr_recv.at[j],
            device_id={"rep": target},
            device_id_type=MESH,
        )

    def spread_copy(j, owner):
        return pltpu.make_async_remote_copy(
            src_ref=own_mean_ref,
            dst_ref=all_mean_ref.at[piece(owner)],
            send_sem=fg_send.at[j],
            recv_sem=fg_recv.at[j],
            device_id={"rep": lax.rem(rep + j, n_rep)},
            device_id_type=MESH,
        )

    def start_all(make, low, high):
        def one(j, _):
            make(j).start()
            return 0

        lax.fori_loop(low, high, one, 0)

    def wait_recv_all(make, low, high):
        def one(j, _):
            make(j).wait_recv()
            return 0

        lax.fori_loop(low, high, one, 0)

    def wait_send_all(make, low, high):
        def one(j, _):
            make(j).wait_send()
            return 0

        lax.fori_loop(low, high, one, 0)

    start_all(gather_copy, 0, chunks)
    start_all(scatter_copy, 1, n_rep)

    for copy in weight_copies:
        copy.wait()

    def own_tile(t, _):
        acc_ref[ds(me, rows), ds(t, tile)] = dot(nm_ref[ds(me, rows), :], w_ref[:, ds(t, tile)])
        return 0

    lax.fori_loop(0, total // tile, own_tile, 0)
    acc_ref[ds(peer, rows), :] = jnp.zeros((rows, total), jnp.float32)

    own_piece.wait()
    wait_recv_all(scatter_copy, 1, n_rep)
    summed = pieces_ref[0].astype(jnp.float32)
    for j in range(1, n_rep):
        summed = summed + pieces_ref[j].astype(jnp.float32)
    summed = summed * (1.0 / n_rep)
    own_mean_ref[...] = summed
    all_mean_ref[piece(rep)] = summed
    start_all(lambda j: spread_copy(j, rep), 1, n_rep)

    def arrived(c, _):
        pltpu.make_async_remote_copy(
            src_ref=nm_ref.at[ds(peer, rows), ds(c, cw)],
            dst_ref=nm_ref.at[ds(peer, rows), ds(c, cw)],
            send_sem=ag_send.at[c],
            recv_sem=ag_recv.at[c],
            device_id={"tp": peer},
            device_id_type=MESH,
        ).wait_recv()
        part = nm_ref[ds(peer, rows), ds(c, cw)]

        def one(t, _):
            acc_ref[ds(peer, rows), ds(t, tile)] += dot(part, w_ref[ds(c, cw), ds(t, tile)])
            return 0

        lax.fori_loop(0, total // tile, one, 0)
        return 0

    lax.fori_loop(0, chunks, arrived, 0)

    cosine, sine = cos_ref[...], sin_ref[...]

    def rope_head(source, target, index):
        vector = acc_ref[:, ds(source, HEAD_SIZE)]
        target[:, ds(index, HEAD_SIZE)] = (
            vector * cosine + pltpu.roll(vector, HEAD_SIZE // 2, 1) * sine
        ).astype(jnp.bfloat16)

    heads_q, heads_kv = qw // HEAD_SIZE, kw // HEAD_SIZE
    for h in range(heads_q):
        rope_head(h, q_ref, h)
    for h in range(heads_kv):
        rope_head(heads_q + h, k_ref, h)
    v_ref[...] = acc_ref[:, pl.ds(qw + kw, kw)].astype(jnp.bfloat16)

    sequence = 2 * rows
    group = heads_q // heads_kv
    scale = HEAD_SIZE ** (-0.5)

    def reverse(gradient, block):
        c = cosine[block * rows : (block + 1) * rows]
        s = sine[block * rows : (block + 1) * rows]
        return (gradient * c - pltpu.roll(gradient, HEAD_SIZE // 2, 1) * s).astype(jnp.bfloat16)

    def kv_head(g, _):
        grad_k = [None, None]
        grad_v = [None, None]
        for r in range(group):
            head = ds(g * group + r, HEAD_SIZE)
            for b in range(2):
                keys = (b + 1) * rows
                block = pl.ds(b * rows, rows)
                query = q_ref[block, head]
                out_grad = go_ref[block, head]
                key = k_ref[pl.ds(0, keys), ds(g, HEAD_SIZE)]
                value = v_ref[pl.ds(0, keys), ds(g, HEAD_SIZE)]
                scores = dot(query, key, NT) * scale
                row = lax.broadcasted_iota(jnp.int32, scores.shape, 0) + b * rows
                col = lax.broadcasted_iota(jnp.int32, scores.shape, 1)
                scores = jnp.where(col <= row, scores, -jnp.inf)
                powers = jnp.exp(scores - jnp.max(scores, axis=-1, keepdims=True))
                prob = powers * (1.0 / jnp.sum(powers, axis=-1, keepdims=True))
                grad_prob = dot(out_grad, value, NT)
                inner = jnp.sum(grad_prob * prob, axis=-1, keepdims=True)
                score_low = (prob * (grad_prob - inner) * scale).astype(jnp.bfloat16)
                dq_ref[block, head] = reverse(dot(score_low, key), b)
                part_v = dot(prob.astype(jnp.bfloat16), out_grad, TN)
                part_k = dot(score_low, query, TN)
                for j in range(b + 1):
                    pv = part_v[j * rows : (j + 1) * rows]
                    pk = part_k[j * rows : (j + 1) * rows]
                    grad_v[j] = pv if grad_v[j] is None else grad_v[j] + pv
                    grad_k[j] = pk if grad_k[j] is None else grad_k[j] + pk
        for j in range(2):
            block = pl.ds(j * rows, rows)
            dk_ref[block, ds(g, HEAD_SIZE)] = reverse(grad_k[j], j)
            dv_ref[block, ds(g, HEAD_SIZE)] = grad_v[j].astype(jnp.bfloat16)
        return 0

    lax.fori_loop(0, heads_kv, kv_head, 0)

    normed_ref[...] = nm_ref[...]
    wait_recv_all(lambda j: spread_copy(j, lax.rem(rep + n_rep - j, n_rep)), 1, n_rep)
    mean_ref[...] = all_mean_ref[...]
    wait_send_all(gather_copy, 0, chunks)
    wait_send_all(scatter_copy, 1, n_rep)
    wait_send_all(lambda j: spread_copy(j, rep), 1, n_rep)


def pair_body(
    n_rep,
    tokens,
    norm_gain,
    w_query,
    key_weight,
    value_weight,
    attention_gradient,
    global_fragment,
    momentum,
    local_fragment,
):
    rows, width = tokens.shape[1:]
    sequence = 2 * rows
    weight_q, weight_k, weight_v = w_query[0], key_weight[0], value_weight[0]
    qw, kw = weight_q.shape[1], weight_k.shape[1]
    total = qw + 2 * kw
    frag_rows = local_fragment.shape[1]
    piece_rows = 16
    piece_cols = width * frag_rows // piece_rows // n_rep
    chunks = 6
    bf16, f32 = jnp.bfloat16, jnp.float32
    cosine, sine = host_tables(sequence, HEAD_SIZE)
    vmem = pl.BlockSpec(memory_space=pltpu.VMEM)
    anyspace = pl.BlockSpec(memory_space=pl.ANY)
    normed, dq, dk, dv, mean_local = pl.pallas_call(
        functools.partial(front_kernel, n_rep, chunks, 512),
        out_shape=(
            jax.ShapeDtypeStruct((sequence, width), bf16),
            jax.ShapeDtypeStruct((sequence, qw), bf16),
            jax.ShapeDtypeStruct((sequence, kw), bf16),
            jax.ShapeDtypeStruct((sequence, kw), bf16),
            jax.ShapeDtypeStruct((frag_rows, width), f32),
        ),
        in_specs=[vmem, vmem, anyspace, anyspace, anyspace, vmem, vmem, vmem, anyspace],
        out_specs=(vmem,) * 5,
        scratch_shapes=[
            pltpu.VMEM((width, total), bf16),
            pltpu.VMEM((sequence, width), bf16),
            pltpu.VMEM((sequence, total), f32),
            pltpu.VMEM((sequence, qw), bf16),
            pltpu.VMEM((sequence, kw), bf16),
            pltpu.VMEM((sequence, kw), bf16),
            pltpu.VMEM((n_rep, piece_rows, piece_cols), bf16),
            pltpu.VMEM((piece_rows, piece_cols), f32),
            pltpu.VMEM((frag_rows, width), f32),
            pltpu.SemaphoreType.DMA((3,)),
            pltpu.SemaphoreType.DMA((chunks,)),
            pltpu.SemaphoreType.DMA((chunks,)),
            pltpu.SemaphoreType.DMA((n_rep,)),
            pltpu.SemaphoreType.DMA((n_rep,)),
            pltpu.SemaphoreType.DMA((n_rep,)),
            pltpu.SemaphoreType.DMA((n_rep,)),
            pltpu.SemaphoreType.DMA,
        ],
        compiler_params=pltpu.CompilerParams(
            collective_id=0, has_side_effects=True, vmem_limit_bytes=40 * 1024 * 1024
        ),
    )(
        tokens[0],
        norm_gain,
        weight_q,
        weight_k,
        weight_v,
        attention_gradient[0],
        cosine,
        sine,
        local_fragment[0],
    )
    me = lax.axis_index("tp")
    swap = [(0, 1), (1, 0)]

    def half(array, which):
        return lax.dynamic_slice_in_dim(array, which * rows, rows, 0)

    def share(which, low, high):
        partial_value = dot(half(dq, which), weight_q[low:high], NT)
        partial_value = partial_value + dot(half(dk, which), weight_k[low:high], NT)
        partial_value = partial_value + dot(half(dv, which), weight_v[low:high], NT)
        return partial_value.astype(bf16)

    cuts = 2
    step = width // cuts
    away = [share(1 - me, c * step, (c + 1) * step) for c in range(cuts)]
    landed = [lax.ppermute(piece, "tp", swap) for piece in away]
    here = share(me, 0, width)
    far = jnp.concatenate(away, axis=1)
    gain_partial = (
        jnp.sum(
            far.astype(f32) * half(normed, 1 - me).astype(f32)
            + here.astype(f32) * half(normed, me).astype(f32),
            axis=0,
            keepdims=True,
        )
        / norm_gain
    )
    gains_gradient = gain_partial + lax.ppermute(gain_partial, "tp", swap)
    grad_wq = dot(normed, dq, TN).astype(bf16)
    grad_wk = dot(normed, dk, TN).astype(bf16)
    grad_wv = dot(normed, dv, TN).astype(bf16)
    mean_delta = global_fragment - mean_local
    new_momentum = outer_momentum * momentum + mean_delta
    new_global = global_fragment - outer_rate * (mean_delta + outer_momentum * new_momentum)
    summed_rows = here.astype(f32) + jnp.concatenate(landed, axis=1).astype(f32)
    widened_rows = tokens[0].astype(f32)
    inverse_norm = lax.rsqrt(
        jnp.mean(widened_rows * widened_rows, axis=-1, keepdims=True) + epsilon
    )
    normalized_input = widened_rows * inverse_norm
    scaled_rows = summed_rows * norm_gain
    gradient_rows = (
        inverse_norm
        * (
            scaled_rows
            - normalized_input * jnp.mean(scaled_rows * normalized_input, axis=-1, keepdims=True)
        )
    ).astype(bf16)
    return (
        grad_wq[None],
        grad_wk[None],
        grad_wv[None],
        gains_gradient,
        gradient_rows[None],
        new_global,
        new_momentum,
    )


def solution(mesh):
    placed = (
        P("rep", "tp", None),
        P("rep", None),
        P("rep", None, "tp"),
        P("rep", None, "tp"),
        P("rep", None, "tp"),
        P("rep", None, "tp"),
        P("tp", None),
        P("tp", None),
        P("rep", "tp", None),
    )
    paired = mesh.shape["tp"] == 2
    chosen = functools.partial(pair_body, mesh.shape["rep"]) if paired else body
    return jax.shard_map(
        chosen,
        mesh=mesh,
        in_specs=placed,
        out_specs=(
            P("rep", None, "tp"),
            P("rep", None, "tp"),
            P("rep", None, "tp"),
            P("rep", None),
            P("rep", "tp", None),
            P("tp", None),
            P("tp", None),
        ),
        check_vma=False,
    )
```

```python
import functools

import jax
import jax.numpy as jnp
import numpy as np
from jax import lax
from jax.experimental import pallas as pl
from jax.experimental.pallas import tpu as pltpu
from jax.sharding import PartitionSpec as P

MESH = pl.DeviceIdType.MESH

HEAD_SIZE = 128


epsilon = 1e-05
rope_base = 500000.0
outer_rate = 0.7
outer_momentum = 0.9


def rope_tables(sequence_length, width):
    middle = width // 2
    frequency = rope_base ** (-2.0 * jnp.arange(middle, dtype=jnp.float32) / width)
    angles = jnp.arange(sequence_length, dtype=jnp.float32)[:, None] * frequency[None, :]
    angles = jnp.concatenate([angles, angles], axis=1)
    return (jnp.cos(angles)[:, None, :], jnp.sin(angles)[:, None, :])


def rotate(vectors, cosine_table, sine_table):
    middle = vectors.shape[-1] // 2
    turned = jnp.concatenate([-vectors[..., middle:], vectors[..., :middle]], axis=-1)
    return vectors * cosine_table + turned * sine_table


def reverse_rotation(gradient, cosine_table, sine_table):
    middle = gradient.shape[-1] // 2
    shifted = gradient * sine_table
    turned = jnp.concatenate([shifted[..., middle:], -shifted[..., :middle]], axis=-1)
    return gradient * cosine_table + turned


def attention_reverse(query_rows, rotated_keys, values_bfloat, grad_out, block_of_rows):
    sequence_length = query_rows.shape[0]
    score_scale = query_rows.shape[-1] ** (-0.5)

    def one_block(running, block_index):
        acc_key, acc_value = running
        offset = block_index * block_of_rows
        query_block = lax.dynamic_slice_in_dim(query_rows, offset, block_of_rows, 0)
        grad_block = lax.dynamic_slice_in_dim(grad_out, offset, block_of_rows, 0)
        scores = (
            jnp.einsum(
                "qgrd,kgd->grqk", query_block, rotated_keys, preferred_element_type=jnp.float32
            )
            * score_scale
        )
        row_pos = offset + jnp.arange(block_of_rows)
        col_pos = jnp.arange(sequence_length)
        allowed = col_pos[None, :] <= row_pos[:, None]
        scores = jnp.where(allowed, scores, -jnp.inf)
        highest = jnp.max(scores, axis=-1, keepdims=True)
        powers = jnp.exp(scores - highest)
        probability = powers / jnp.sum(powers, axis=-1, keepdims=True)
        prob_low = probability.astype(jnp.bfloat16)
        acc_value = acc_value + jnp.einsum(
            "grqk,qgrd->kgd", prob_low, grad_block, preferred_element_type=jnp.float32
        )
        grad_prob = jnp.einsum(
            "qgrd,kgd->grqk", grad_block, values_bfloat, preferred_element_type=jnp.float32
        )
        grad_score = (
            probability
            * (grad_prob - jnp.sum(grad_prob * probability, axis=-1, keepdims=True))
            * score_scale
        )
        score_low = grad_score.astype(jnp.bfloat16)
        grad_query = jnp.einsum(
            "grqk,kgd->qgrd", score_low, rotated_keys, preferred_element_type=jnp.float32
        )
        acc_key = acc_key + jnp.einsum(
            "grqk,qgrd->kgd", score_low, query_block, preferred_element_type=jnp.float32
        )
        return ((acc_key, acc_value), grad_query)

    initial = jnp.zeros(rotated_keys.shape, jnp.float32)
    (acc_key, acc_value), grad_blocks = lax.scan(
        one_block, (initial, initial), jnp.arange(sequence_length // block_of_rows)
    )
    return (grad_blocks.reshape(query_rows.shape), acc_key, acc_value)


def body(
    tokens,
    norm_gain,
    w_query,
    key_weight,
    value_weight,
    attention_gradient,
    global_fragment,
    momentum,
    local_fragment,
):
    local_rows = tokens[0]
    norm_gains = norm_gain[0]
    weight_q = w_query[0]
    weight_k = key_weight[0]
    weight_v = value_weight[0]
    widened_rows = local_rows.astype(jnp.float32)
    inverse_norm = lax.rsqrt(
        jnp.mean(widened_rows * widened_rows, axis=-1, keepdims=True) + epsilon
    )
    normalized_input = widened_rows * inverse_norm
    normalized_local = (normalized_input * norm_gains[None, :]).astype(jnp.bfloat16)
    normalized = lax.all_gather(normalized_local, "tp", axis=0, tiled=True)
    sequence_length = normalized.shape[0]
    heads_q = weight_q.shape[1] // HEAD_SIZE
    heads_kv = weight_k.shape[1] // HEAD_SIZE
    cosine_table, sine_table = rope_tables(sequence_length, HEAD_SIZE)
    query_rows = jnp.dot(normalized, weight_q, preferred_element_type=jnp.float32).reshape(
        sequence_length, heads_q, HEAD_SIZE
    )
    query_rows = rotate(query_rows, cosine_table, sine_table).astype(jnp.bfloat16)
    rotated_keys = jnp.dot(normalized, weight_k, preferred_element_type=jnp.float32).reshape(
        sequence_length, heads_kv, HEAD_SIZE
    )
    rotated_keys = rotate(rotated_keys, cosine_table, sine_table).astype(jnp.bfloat16)
    values_bfloat = (
        jnp.dot(normalized, weight_v, preferred_element_type=jnp.float32)
        .astype(jnp.bfloat16)
        .reshape(sequence_length, heads_kv, HEAD_SIZE)
    )
    replica_group = heads_q // heads_kv
    block_of_rows = min(512, sequence_length)
    query_input_gradient, key_input_gradient, value_input_gradient = attention_reverse(
        query_rows.reshape(sequence_length, heads_kv, replica_group, HEAD_SIZE),
        rotated_keys,
        values_bfloat,
        attention_gradient[0].reshape(sequence_length, heads_kv, replica_group, HEAD_SIZE),
        block_of_rows,
    )
    dquery = (
        reverse_rotation(
            query_input_gradient.reshape(sequence_length, heads_q, HEAD_SIZE),
            cosine_table,
            sine_table,
        )
        .astype(jnp.bfloat16)
        .reshape(sequence_length, heads_q * HEAD_SIZE)
    )
    key_gradient = (
        reverse_rotation(key_input_gradient, cosine_table, sine_table)
        .astype(jnp.bfloat16)
        .reshape(sequence_length, heads_kv * HEAD_SIZE)
    )
    value_gradient = value_input_gradient.astype(jnp.bfloat16).reshape(
        sequence_length, heads_kv * HEAD_SIZE
    )
    contract = (((0,), (0,)), ((), ()))
    grad_wq = lax.dot_general(
        normalized, dquery, contract, preferred_element_type=jnp.float32
    ).astype(jnp.bfloat16)
    grad_wk = lax.dot_general(
        normalized, key_gradient, contract, preferred_element_type=jnp.float32
    ).astype(jnp.bfloat16)
    grad_wv = lax.dot_general(
        normalized, value_gradient, contract, preferred_element_type=jnp.float32
    ).astype(jnp.bfloat16)
    back = (((1,), (1,)), ((), ()))
    partial_value = lax.dot_general(dquery, weight_q, back, preferred_element_type=jnp.float32)
    partial_value = partial_value + lax.dot_general(
        key_gradient, weight_k, back, preferred_element_type=jnp.float32
    )
    summed_rows = lax.psum_scatter(
        (
            partial_value
            + lax.dot_general(value_gradient, weight_v, back, preferred_element_type=jnp.float32)
        ).astype(jnp.bfloat16),
        "tp",
        scatter_dimension=0,
        tiled=True,
    ).astype(jnp.float32)
    gains_gradient = lax.psum(jnp.sum(summed_rows * normalized_input, axis=0), "tp")
    scaled_rows = summed_rows * norm_gains[None, :]
    gradient_rows = (
        inverse_norm
        * (
            scaled_rows
            - normalized_input * jnp.mean(scaled_rows * normalized_input, axis=-1, keepdims=True)
        )
    ).astype(jnp.bfloat16)
    delta = global_fragment - local_fragment[0].astype(jnp.float32)
    replicas = lax.axis_size("rep")
    mean_delta = lax.psum(delta, "rep") / replicas
    new_momentum = outer_momentum * momentum + mean_delta
    new_global = global_fragment - outer_rate * (mean_delta + outer_momentum * new_momentum)
    return (
        grad_wq[None],
        grad_wk[None],
        grad_wv[None],
        gains_gradient[None],
        gradient_rows[None],
        new_global,
        new_momentum,
    )

NT = (((1,), (1,)), ((), ()))
TN = (((0,), (0,)), ((), ()))


def dot(a, b, dims=(((1,), (0,)), ((), ()))):
    return lax.dot_general(a, b, dims, preferred_element_type=jnp.float32)


def ds(index, size):
    return pl.ds(pl.multiple_of(index * size, size), size)


def host_tables(sequence_length, width):
    middle = width // 2
    frequency = rope_base ** (-2.0 * np.arange(middle) / width)
    angles = np.arange(sequence_length)[:, None] * frequency[None, :]
    cosine, sine = np.cos(angles), np.sin(angles)
    return (
        jnp.asarray(np.concatenate([cosine, cosine], axis=1), jnp.float32),
        jnp.asarray(np.concatenate([-sine, sine], axis=1), jnp.float32),
    )


def front_kernel(
    n_rep,
    chunks,
    tile,
    tokens_hbm,
    gain_hbm,
    wq_hbm,
    wk_hbm,
    wv_hbm,
    go_hbm,
    cos_hbm,
    sin_hbm,
    local_hbm,
    normed_hbm,
    grads_hbm,
    away_hbm,
    mean_hbm,
    tokens_ref,
    gain_ref,
    go_ref,
    cos_ref,
    sin_ref,
    w_ref,
    nm_ref,
    acc_ref,
    q_ref,
    k_ref,
    v_ref,
    grads_ref,
    away_ref,
    pieces_ref,
    own_mean_ref,
    all_mean_ref,
    in_sems,
    out_sems,
    away_sems,
    w_sems,
    ag_send,
    ag_recv,
    fr_send,
    fr_recv,
    fg_send,
    fg_recv,
    own_sem,
):
    me = lax.axis_index("tp")
    peer = 1 - me
    rep = lax.axis_index("rep")
    rows, width = tokens_ref.shape
    qw, kw = wq_hbm.shape[1], wk_hbm.shape[1]
    total = qw + 2 * kw
    cw = width // chunks
    piece_rows, piece_cols = own_mean_ref.shape
    col_blocks = width // piece_cols
    loads = [
        pltpu.make_async_copy(source, target, in_sems.at[i])
        for i, (source, target) in enumerate(
            (
                (tokens_hbm, tokens_ref),
                (gain_hbm, gain_ref),
                (cos_hbm, cos_ref),
                (sin_hbm, sin_ref),
                (go_hbm, go_ref),
            )
        )
    ]
    for copy in loads:
        copy.start()
    barrier = pltpu.get_barrier_semaphore()
    pl.semaphore_signal(barrier, inc=1, device_id={"tp": peer}, device_id_type=MESH)

    def greet(j, _):
        pl.semaphore_signal(
            barrier, inc=1, device_id={"rep": lax.rem(rep + j, n_rep)}, device_id_type=MESH
        )
        return 0

    lax.fori_loop(1, n_rep, greet, 0)
    weight_copies = [
        pltpu.make_async_copy(wq_hbm, w_ref.at[:, pl.ds(0, qw)], w_sems.at[0]),
        pltpu.make_async_copy(wk_hbm, w_ref.at[:, pl.ds(qw, kw)], w_sems.at[1]),
        pltpu.make_async_copy(wv_hbm, w_ref.at[:, pl.ds(qw + kw, kw)], w_sems.at[2]),
    ]
    for copy in weight_copies:
        copy.start()

    def piece(owner):
        return (
            ds(owner // col_blocks, piece_rows),
            ds(lax.rem(owner, col_blocks), piece_cols),
        )

    own_piece = pltpu.make_async_copy(local_hbm.at[piece(rep)], pieces_ref.at[0], own_sem)
    own_piece.start()

    for copy in loads:
        copy.wait()
    step = 16

    def norm_rows(i, _):
        x = tokens_ref[ds(i, step), :].astype(jnp.float32)
        inverse = lax.rsqrt(jnp.mean(x * x, axis=-1, keepdims=True) + epsilon)
        nm_ref[pl.ds(pl.multiple_of(me * rows + i * step, step), step), :] = (
            x * inverse * gain_ref[...]
        ).astype(jnp.bfloat16)
        return 0

    lax.fori_loop(0, rows // step, norm_rows, 0)
    pl.semaphore_wait(barrier, n_rep)

    def gather_copy(c):
        part = nm_ref.at[ds(me, rows), ds(c, cw)]
        return pltpu.make_async_remote_copy(
            src_ref=part,
            dst_ref=part,
            send_sem=ag_send.at[c],
            recv_sem=ag_recv.at[c],
            device_id={"tp": peer},
            device_id_type=MESH,
        )

    def scatter_copy(j):
        target = lax.rem(rep + j, n_rep)
        return pltpu.make_async_remote_copy(
            src_ref=local_hbm.at[piece(target)],
            dst_ref=pieces_ref.at[j],
            send_sem=fr_send.at[j],
            recv_sem=fr_recv.at[j],
            device_id={"rep": target},
            device_id_type=MESH,
        )

    def spread_copy(j, owner):
        return pltpu.make_async_remote_copy(
            src_ref=own_mean_ref,
            dst_ref=all_mean_ref.at[piece(owner)],
            send_sem=fg_send.at[j],
            recv_sem=fg_recv.at[j],
            device_id={"rep": lax.rem(rep + j, n_rep)},
            device_id_type=MESH,
        )

    def start_all(make, low, high):
        def one(j, _):
            make(j).start()
            return 0

        lax.fori_loop(low, high, one, 0)

    def wait_recv_all(make, low, high):
        def one(j, _):
            make(j).wait_recv()
            return 0

        lax.fori_loop(low, high, one, 0)

    def wait_send_all(make, low, high):
        def one(j, _):
            make(j).wait_send()
            return 0

        lax.fori_loop(low, high, one, 0)

    start_all(gather_copy, 0, chunks)
    start_all(scatter_copy, 1, n_rep)

    for copy in weight_copies:
        copy.wait()

    def own_tile(t, _):
        acc_ref[ds(me, rows), ds(t, tile)] = dot(nm_ref[ds(me, rows), :], w_ref[:, ds(t, tile)])
        return 0

    lax.fori_loop(0, total // tile, own_tile, 0)
    acc_ref[ds(peer, rows), :] = jnp.zeros((rows, total), jnp.float32)

    own_piece.wait()
    wait_recv_all(scatter_copy, 1, n_rep)
    summed = pieces_ref[0].astype(jnp.float32)
    for j in range(1, n_rep):
        summed = summed + pieces_ref[j].astype(jnp.float32)
    summed = summed * (1.0 / n_rep)
    own_mean_ref[...] = summed
    all_mean_ref[piece(rep)] = summed
    start_all(lambda j: spread_copy(j, rep), 1, n_rep)

    def arrived(c, _):
        pltpu.make_async_remote_copy(
            src_ref=nm_ref.at[ds(peer, rows), ds(c, cw)],
            dst_ref=nm_ref.at[ds(peer, rows), ds(c, cw)],
            send_sem=ag_send.at[c],
            recv_sem=ag_recv.at[c],
            device_id={"tp": peer},
            device_id_type=MESH,
        ).wait_recv()
        part = nm_ref[ds(peer, rows), ds(c, cw)]

        def one(t, _):
            acc_ref[ds(peer, rows), ds(t, tile)] += dot(part, w_ref[ds(c, cw), ds(t, tile)])
            return 0

        lax.fori_loop(0, total // tile, one, 0)
        return 0

    lax.fori_loop(0, chunks, arrived, 0)

    normed_out = pltpu.make_async_copy(nm_ref, normed_hbm, out_sems.at[0])
    normed_out.start()
    cosine, sine = cos_ref[...], sin_ref[...]

    def rope_head(source, target, index):
        vector = acc_ref[:, ds(source, HEAD_SIZE)]
        target[:, ds(index, HEAD_SIZE)] = (
            vector * cosine + pltpu.roll(vector, HEAD_SIZE // 2, 1) * sine
        ).astype(jnp.bfloat16)

    heads_q, heads_kv = qw // HEAD_SIZE, kw // HEAD_SIZE
    for h in range(heads_q):
        rope_head(h, q_ref, h)
    for h in range(heads_kv):
        rope_head(heads_q + h, k_ref, h)
    v_ref[...] = acc_ref[:, pl.ds(qw + kw, kw)].astype(jnp.bfloat16)

    sequence = 2 * rows
    group = heads_q // heads_kv
    scale = HEAD_SIZE ** (-0.5)

    def reverse(gradient, block):
        c = cosine[block * rows : (block + 1) * rows]
        s = sine[block * rows : (block + 1) * rows]
        return (gradient * c - pltpu.roll(gradient, HEAD_SIZE // 2, 1) * s).astype(jnp.bfloat16)

    def kv_head(g, _):
        grad_k = [None, None]
        grad_v = [None, None]
        for r in range(group):
            head = ds(g * group + r, HEAD_SIZE)
            for b in range(2):
                keys = (b + 1) * rows
                block = pl.ds(b * rows, rows)
                query = q_ref[block, head]
                out_grad = go_ref[block, head]
                key = k_ref[pl.ds(0, keys), ds(g, HEAD_SIZE)]
                value = v_ref[pl.ds(0, keys), ds(g, HEAD_SIZE)]
                scores = dot(query, key, NT) * scale
                row = lax.broadcasted_iota(jnp.int32, scores.shape, 0) + b * rows
                col = lax.broadcasted_iota(jnp.int32, scores.shape, 1)
                scores = jnp.where(col <= row, scores, -jnp.inf)
                powers = jnp.exp(scores - jnp.max(scores, axis=-1, keepdims=True))
                prob = powers * (1.0 / jnp.sum(powers, axis=-1, keepdims=True))
                grad_prob = dot(out_grad, value, NT)
                inner = jnp.sum(grad_prob * prob, axis=-1, keepdims=True)
                score_low = (prob * (grad_prob - inner) * scale).astype(jnp.bfloat16)
                grads_ref[block, head] = reverse(dot(score_low, key), b)
                part_v = dot(prob.astype(jnp.bfloat16), out_grad, TN)
                part_k = dot(score_low, query, TN)
                for j in range(b + 1):
                    pv = part_v[j * rows : (j + 1) * rows]
                    pk = part_k[j * rows : (j + 1) * rows]
                    grad_v[j] = pv if grad_v[j] is None else grad_v[j] + pv
                    grad_k[j] = pk if grad_k[j] is None else grad_k[j] + pk
        for j in range(2):
            block = pl.ds(j * rows, rows)
            grads_ref[block, ds(heads_q + g, HEAD_SIZE)] = reverse(grad_k[j], j)
            grads_ref[block, ds(heads_q + heads_kv + g, HEAD_SIZE)] = grad_v[j].astype(jnp.bfloat16)
        return 0

    lax.fori_loop(0, heads_kv, kv_head, 0)

    grads_out = pltpu.make_async_copy(grads_ref, grads_hbm, out_sems.at[1])
    grads_out.start()
    wait_recv_all(lambda j: spread_copy(j, lax.rem(rep + n_rep - j, n_rep)), 1, n_rep)
    mean_out = pltpu.make_async_copy(all_mean_ref, mean_hbm, out_sems.at[2])
    mean_out.start()

    def away_copy(c):
        columns = ds(c, cw)
        return pltpu.make_async_copy(
            away_ref.at[:, columns], away_hbm.at[:, columns], away_sems.at[c]
        )

    def share(c, _):
        away_ref[:, ds(c, cw)] = dot(
            grads_ref[ds(peer, rows), :], w_ref[ds(c, cw), :], NT
        ).astype(jnp.bfloat16)
        away_copy(c).start()
        return 0

    lax.fori_loop(0, chunks, share, 0)
    wait_send_all(gather_copy, 0, chunks)
    wait_send_all(scatter_copy, 1, n_rep)
    wait_send_all(lambda j: spread_copy(j, rep), 1, n_rep)
    normed_out.wait()
    grads_out.wait()
    mean_out.wait()
    for c in range(chunks):
        away_copy(c).wait()


def weight_kernel(
    rows,
    normed_ref,
    grads_ref,
    away_ref,
    gain_ref,
    wq_ref,
    wk_ref,
    wv_ref,
    global_ref,
    momentum_ref,
    mean_ref,
    dwq_ref,
    dwk_ref,
    dwv_ref,
    here_ref,
    gain_out,
    new_global,
    new_momentum,
):
    me = lax.axis_index("tp")
    qw, kw = wq_ref.shape[1], wk_ref.shape[1]
    own = ds(me, rows)
    here = dot(grads_ref[own, pl.ds(0, qw)], wq_ref[...], NT)
    here = here + dot(grads_ref[own, pl.ds(qw, kw)], wk_ref[...], NT)
    here = here + dot(grads_ref[own, pl.ds(qw + kw, kw)], wv_ref[...], NT)
    here = here.astype(jnp.bfloat16)
    here_ref[...] = here
    normed = normed_ref[...]
    dwq_ref[...] = dot(normed, grads_ref[:, pl.ds(0, qw)], TN).astype(jnp.bfloat16)
    dwk_ref[...] = dot(normed, grads_ref[:, pl.ds(qw, kw)], TN).astype(jnp.bfloat16)
    dwv_ref[...] = dot(normed, grads_ref[:, pl.ds(qw + kw, kw)], TN).astype(jnp.bfloat16)
    products = here.astype(jnp.float32) * normed_ref[own, :].astype(jnp.float32)
    products += away_ref[...].astype(jnp.float32) * normed_ref[ds(1 - me, rows), :].astype(
        jnp.float32
    )
    gain_out[...] = jnp.sum(products, axis=0, keepdims=True) / gain_ref[...]
    outer = global_ref[...]
    mean_delta = outer - mean_ref[...]
    updated = outer_momentum * momentum_ref[...] + mean_delta
    new_momentum[...] = updated
    new_global[...] = outer - outer_rate * (mean_delta + outer_momentum * updated)


def tail_kernel(tokens_ref, gain_ref, here_ref, landed_ref, mine_ref, other_ref, out_ref, total_ref):
    x = tokens_ref[...].astype(jnp.float32)
    inverse = lax.rsqrt(jnp.mean(x * x, axis=-1, keepdims=True) + epsilon)
    xhat = x * inverse
    band = tokens_ref.shape[0]
    landed = landed_ref[ds(pl.program_id(0), band), :].astype(jnp.float32)
    scaled = (here_ref[...].astype(jnp.float32) + landed) * gain_ref[...]
    inner = jnp.mean(scaled * xhat, axis=-1, keepdims=True)
    out_ref[...] = (inverse * (scaled - xhat * inner)).astype(jnp.bfloat16)
    total_ref[...] = mine_ref[...] + other_ref[...]


def pair_body(
    n_rep,
    tokens,
    norm_gain,
    w_query,
    key_weight,
    value_weight,
    attention_gradient,
    global_fragment,
    momentum,
    local_fragment,
):
    rows, width = tokens.shape[1:]
    sequence = 2 * rows
    weight_q, weight_k, weight_v = w_query[0], key_weight[0], value_weight[0]
    qw, kw = weight_q.shape[1], weight_k.shape[1]
    total = qw + 2 * kw
    frag_rows = local_fragment.shape[1]
    piece_rows = 16
    piece_cols = width * frag_rows // piece_rows // n_rep
    chunks = 6
    bf16, f32 = jnp.bfloat16, jnp.float32
    cosine, sine = host_tables(sequence, HEAD_SIZE)
    vmem = pl.BlockSpec(memory_space=pltpu.VMEM)
    anyspace = pl.BlockSpec(memory_space=pl.ANY)
    normed, grads, away, mean_local = pl.pallas_call(
        functools.partial(front_kernel, n_rep, chunks, 512),
        out_shape=(
            jax.ShapeDtypeStruct((sequence, width), bf16),
            jax.ShapeDtypeStruct((sequence, total), bf16),
            jax.ShapeDtypeStruct((rows, width), bf16),
            jax.ShapeDtypeStruct((frag_rows, width), f32),
        ),
        in_specs=[anyspace] * 9,
        out_specs=(anyspace,) * 4,
        scratch_shapes=[
            pltpu.VMEM((rows, width), bf16),
            pltpu.VMEM((1, width), f32),
            pltpu.VMEM((sequence, qw), bf16),
            pltpu.VMEM((sequence, HEAD_SIZE), f32),
            pltpu.VMEM((sequence, HEAD_SIZE), f32),
            pltpu.VMEM((width, total), bf16),
            pltpu.VMEM((sequence, width), bf16),
            pltpu.VMEM((sequence, total), f32),
            pltpu.VMEM((sequence, qw), bf16),
            pltpu.VMEM((sequence, kw), bf16),
            pltpu.VMEM((sequence, kw), bf16),
            pltpu.VMEM((sequence, total), bf16),
            pltpu.VMEM((rows, width), bf16),
            pltpu.VMEM((n_rep, piece_rows, piece_cols), bf16),
            pltpu.VMEM((piece_rows, piece_cols), f32),
            pltpu.VMEM((frag_rows, width), f32),
            pltpu.SemaphoreType.DMA((5,)),
            pltpu.SemaphoreType.DMA((3,)),
            pltpu.SemaphoreType.DMA((chunks,)),
            pltpu.SemaphoreType.DMA((3,)),
            pltpu.SemaphoreType.DMA((chunks,)),
            pltpu.SemaphoreType.DMA((chunks,)),
            pltpu.SemaphoreType.DMA((n_rep,)),
            pltpu.SemaphoreType.DMA((n_rep,)),
            pltpu.SemaphoreType.DMA((n_rep,)),
            pltpu.SemaphoreType.DMA((n_rep,)),
            pltpu.SemaphoreType.DMA,
        ],
        compiler_params=pltpu.CompilerParams(
            collective_id=0, has_side_effects=True, vmem_limit_bytes=60 * 1024 * 1024
        ),
    )(
        tokens[0],
        norm_gain,
        weight_q,
        weight_k,
        weight_v,
        attention_gradient[0],
        cosine,
        sine,
        local_fragment[0],
    )
    swap = [(0, 1), (1, 0)]
    landed = lax.ppermute(away, "tp", swap)
    cw = width // chunks

    def columns(height):
        return pl.BlockSpec((height, cw), lambda i: (0, i))

    def rows_of(breadth):
        return pl.BlockSpec((cw, breadth), lambda i: (i, 0))

    grad_wq, grad_wk, grad_wv, here, gain_partial, new_global, new_momentum = pl.pallas_call(
        functools.partial(weight_kernel, rows),
        grid=(chunks,),
        out_shape=(
            jax.ShapeDtypeStruct((width, qw), bf16),
            jax.ShapeDtypeStruct((width, kw), bf16),
            jax.ShapeDtypeStruct((width, kw), bf16),
            jax.ShapeDtypeStruct((rows, width), bf16),
            jax.ShapeDtypeStruct((1, width), f32),
            jax.ShapeDtypeStruct((frag_rows, width), f32),
            jax.ShapeDtypeStruct((frag_rows, width), f32),
        ),
        in_specs=[
            columns(sequence),
            pl.BlockSpec((sequence, total), lambda i: (0, 0)),
            columns(rows),
            columns(1),
            rows_of(qw),
            rows_of(kw),
            rows_of(kw),
            columns(frag_rows),
            columns(frag_rows),
            columns(frag_rows),
        ],
        out_specs=(
            rows_of(qw),
            rows_of(kw),
            rows_of(kw),
            columns(rows),
            columns(1),
            columns(frag_rows),
            columns(frag_rows),
        ),
        compiler_params=pltpu.CompilerParams(vmem_limit_bytes=60 * 1024 * 1024),
        cost_estimate=pl.CostEstimate(
            flops=6 * sequence * width * total // 2,
            bytes_accessed=4 * width * total + 12 * frag_rows * width * 2,
            transcendentals=0,
        ),
    )(
        normed,
        grads,
        away,
        norm_gain,
        weight_q,
        weight_k,
        weight_v,
        global_fragment,
        momentum,
        mean_local,
    )
    gain_other = lax.ppermute(gain_partial, "tp", swap)
    band = 32
    row_block = pl.BlockSpec((band, width), lambda i: (i, 0))
    whole_row = pl.BlockSpec((1, width), lambda i: (0, 0))
    gradient_rows, gains_gradient = pl.pallas_call(
        tail_kernel,
        grid=(rows // band,),
        out_shape=(
            jax.ShapeDtypeStruct((rows, width), bf16),
            jax.ShapeDtypeStruct((1, width), f32),
        ),
        in_specs=[row_block, whole_row, row_block, vmem, vmem, vmem],
        out_specs=(row_block, whole_row),
        compiler_params=pltpu.CompilerParams(vmem_limit_bytes=16 * 1024 * 1024),
        cost_estimate=pl.CostEstimate(
            flops=10 * rows * width, bytes_accessed=8 * rows * width, transcendentals=0
        ),
    )(tokens[0], norm_gain, here, landed, gain_partial, gain_other)
    return (
        grad_wq[None],
        grad_wk[None],
        grad_wv[None],
        gains_gradient,
        gradient_rows[None],
        new_global,
        new_momentum,
    )


def solution(mesh):
    placed = (
        P("rep", "tp", None),
        P("rep", None),
        P("rep", None, "tp"),
        P("rep", None, "tp"),
        P("rep", None, "tp"),
        P("rep", None, "tp"),
        P("tp", None),
        P("tp", None),
        P("rep", "tp", None),
    )
    paired = mesh.shape["tp"] == 2
    chosen = functools.partial(pair_body, mesh.shape["rep"]) if paired else body
    return jax.shard_map(
        chosen,
        mesh=mesh,
        in_specs=placed,
        out_specs=(
            P("rep", None, "tp"),
            P("rep", None, "tp"),
            P("rep", None, "tp"),
            P("rep", None),
            P("rep", "tp", None),
            P("tp", None),
            P("tp", None),
        ),
        check_vma=False,
    )
```

```python
import functools

import jax
import jax.numpy as jnp
import numpy as np
from jax import lax
from jax.experimental import pallas as pl
from jax.experimental.pallas import tpu as pltpu
from jax.sharding import PartitionSpec as P

MESH = pl.DeviceIdType.MESH

HEAD_SIZE = 128


epsilon = 1e-05
rope_base = 500000.0
outer_rate = 0.7
outer_momentum = 0.9


def rope_tables(sequence_length, width):
    middle = width // 2
    frequency = rope_base ** (-2.0 * jnp.arange(middle, dtype=jnp.float32) / width)
    angles = jnp.arange(sequence_length, dtype=jnp.float32)[:, None] * frequency[None, :]
    angles = jnp.concatenate([angles, angles], axis=1)
    return (jnp.cos(angles)[:, None, :], jnp.sin(angles)[:, None, :])


def rotate(vectors, cosine_table, sine_table):
    middle = vectors.shape[-1] // 2
    turned = jnp.concatenate([-vectors[..., middle:], vectors[..., :middle]], axis=-1)
    return vectors * cosine_table + turned * sine_table


def reverse_rotation(gradient, cosine_table, sine_table):
    middle = gradient.shape[-1] // 2
    shifted = gradient * sine_table
    turned = jnp.concatenate([shifted[..., middle:], -shifted[..., :middle]], axis=-1)
    return gradient * cosine_table + turned


def attention_reverse(query_rows, rotated_keys, values_bfloat, grad_out, block_of_rows):
    sequence_length = query_rows.shape[0]
    score_scale = query_rows.shape[-1] ** (-0.5)

    def one_block(running, block_index):
        acc_key, acc_value = running
        offset = block_index * block_of_rows
        query_block = lax.dynamic_slice_in_dim(query_rows, offset, block_of_rows, 0)
        grad_block = lax.dynamic_slice_in_dim(grad_out, offset, block_of_rows, 0)
        scores = (
            jnp.einsum(
                "qgrd,kgd->grqk", query_block, rotated_keys, preferred_element_type=jnp.float32
            )
            * score_scale
        )
        row_pos = offset + jnp.arange(block_of_rows)
        col_pos = jnp.arange(sequence_length)
        allowed = col_pos[None, :] <= row_pos[:, None]
        scores = jnp.where(allowed, scores, -jnp.inf)
        highest = jnp.max(scores, axis=-1, keepdims=True)
        powers = jnp.exp(scores - highest)
        probability = powers / jnp.sum(powers, axis=-1, keepdims=True)
        prob_low = probability.astype(jnp.bfloat16)
        acc_value = acc_value + jnp.einsum(
            "grqk,qgrd->kgd", prob_low, grad_block, preferred_element_type=jnp.float32
        )
        grad_prob = jnp.einsum(
            "qgrd,kgd->grqk", grad_block, values_bfloat, preferred_element_type=jnp.float32
        )
        grad_score = (
            probability
            * (grad_prob - jnp.sum(grad_prob * probability, axis=-1, keepdims=True))
            * score_scale
        )
        score_low = grad_score.astype(jnp.bfloat16)
        grad_query = jnp.einsum(
            "grqk,kgd->qgrd", score_low, rotated_keys, preferred_element_type=jnp.float32
        )
        acc_key = acc_key + jnp.einsum(
            "grqk,qgrd->kgd", score_low, query_block, preferred_element_type=jnp.float32
        )
        return ((acc_key, acc_value), grad_query)

    initial = jnp.zeros(rotated_keys.shape, jnp.float32)
    (acc_key, acc_value), grad_blocks = lax.scan(
        one_block, (initial, initial), jnp.arange(sequence_length // block_of_rows)
    )
    return (grad_blocks.reshape(query_rows.shape), acc_key, acc_value)


def body(
    tokens,
    norm_gain,
    w_query,
    key_weight,
    value_weight,
    attention_gradient,
    global_fragment,
    momentum,
    local_fragment,
):
    local_rows = tokens[0]
    norm_gains = norm_gain[0]
    weight_q = w_query[0]
    weight_k = key_weight[0]
    weight_v = value_weight[0]
    widened_rows = local_rows.astype(jnp.float32)
    inverse_norm = lax.rsqrt(
        jnp.mean(widened_rows * widened_rows, axis=-1, keepdims=True) + epsilon
    )
    normalized_input = widened_rows * inverse_norm
    normalized_local = (normalized_input * norm_gains[None, :]).astype(jnp.bfloat16)
    normalized = lax.all_gather(normalized_local, "tp", axis=0, tiled=True)
    sequence_length = normalized.shape[0]
    heads_q = weight_q.shape[1] // HEAD_SIZE
    heads_kv = weight_k.shape[1] // HEAD_SIZE
    cosine_table, sine_table = rope_tables(sequence_length, HEAD_SIZE)
    query_rows = jnp.dot(normalized, weight_q, preferred_element_type=jnp.float32).reshape(
        sequence_length, heads_q, HEAD_SIZE
    )
    query_rows = rotate(query_rows, cosine_table, sine_table).astype(jnp.bfloat16)
    rotated_keys = jnp.dot(normalized, weight_k, preferred_element_type=jnp.float32).reshape(
        sequence_length, heads_kv, HEAD_SIZE
    )
    rotated_keys = rotate(rotated_keys, cosine_table, sine_table).astype(jnp.bfloat16)
    values_bfloat = (
        jnp.dot(normalized, weight_v, preferred_element_type=jnp.float32)
        .astype(jnp.bfloat16)
        .reshape(sequence_length, heads_kv, HEAD_SIZE)
    )
    replica_group = heads_q // heads_kv
    block_of_rows = min(512, sequence_length)
    query_input_gradient, key_input_gradient, value_input_gradient = attention_reverse(
        query_rows.reshape(sequence_length, heads_kv, replica_group, HEAD_SIZE),
        rotated_keys,
        values_bfloat,
        attention_gradient[0].reshape(sequence_length, heads_kv, replica_group, HEAD_SIZE),
        block_of_rows,
    )
    dquery = (
        reverse_rotation(
            query_input_gradient.reshape(sequence_length, heads_q, HEAD_SIZE),
            cosine_table,
            sine_table,
        )
        .astype(jnp.bfloat16)
        .reshape(sequence_length, heads_q * HEAD_SIZE)
    )
    key_gradient = (
        reverse_rotation(key_input_gradient, cosine_table, sine_table)
        .astype(jnp.bfloat16)
        .reshape(sequence_length, heads_kv * HEAD_SIZE)
    )
    value_gradient = value_input_gradient.astype(jnp.bfloat16).reshape(
        sequence_length, heads_kv * HEAD_SIZE
    )
    contract = (((0,), (0,)), ((), ()))
    grad_wq = lax.dot_general(
        normalized, dquery, contract, preferred_element_type=jnp.float32
    ).astype(jnp.bfloat16)
    grad_wk = lax.dot_general(
        normalized, key_gradient, contract, preferred_element_type=jnp.float32
    ).astype(jnp.bfloat16)
    grad_wv = lax.dot_general(
        normalized, value_gradient, contract, preferred_element_type=jnp.float32
    ).astype(jnp.bfloat16)
    back = (((1,), (1,)), ((), ()))
    partial_value = lax.dot_general(dquery, weight_q, back, preferred_element_type=jnp.float32)
    partial_value = partial_value + lax.dot_general(
        key_gradient, weight_k, back, preferred_element_type=jnp.float32
    )
    summed_rows = lax.psum_scatter(
        (
            partial_value
            + lax.dot_general(value_gradient, weight_v, back, preferred_element_type=jnp.float32)
        ).astype(jnp.bfloat16),
        "tp",
        scatter_dimension=0,
        tiled=True,
    ).astype(jnp.float32)
    gains_gradient = lax.psum(jnp.sum(summed_rows * normalized_input, axis=0), "tp")
    scaled_rows = summed_rows * norm_gains[None, :]
    gradient_rows = (
        inverse_norm
        * (
            scaled_rows
            - normalized_input * jnp.mean(scaled_rows * normalized_input, axis=-1, keepdims=True)
        )
    ).astype(jnp.bfloat16)
    delta = global_fragment - local_fragment[0].astype(jnp.float32)
    replicas = lax.axis_size("rep")
    mean_delta = lax.psum(delta, "rep") / replicas
    new_momentum = outer_momentum * momentum + mean_delta
    new_global = global_fragment - outer_rate * (mean_delta + outer_momentum * new_momentum)
    return (
        grad_wq[None],
        grad_wk[None],
        grad_wv[None],
        gains_gradient[None],
        gradient_rows[None],
        new_global,
        new_momentum,
    )

NT = (((1,), (1,)), ((), ()))
TN = (((0,), (0,)), ((), ()))


def dot(a, b, dims=(((1,), (0,)), ((), ()))):
    return lax.dot_general(a, b, dims, preferred_element_type=jnp.float32)


def ds(index, size):
    return pl.ds(pl.multiple_of(index * size, size), size)


def host_tables(sequence_length, width):
    middle = width // 2
    frequency = rope_base ** (-2.0 * np.arange(middle) / width)
    angles = np.arange(sequence_length)[:, None] * frequency[None, :]
    cosine, sine = np.cos(angles), np.sin(angles)
    return (
        jnp.asarray(np.concatenate([cosine, cosine], axis=1), jnp.float32),
        jnp.asarray(np.concatenate([-sine, sine], axis=1), jnp.float32),
    )


def front_kernel(
    n_rep,
    chunks,
    tile,
    tokens_hbm,
    gain_hbm,
    wq_hbm,
    wk_hbm,
    wv_hbm,
    go_hbm,
    cos_hbm,
    sin_hbm,
    local_hbm,
    outer_hbm,
    normed_hbm,
    grads_hbm,
    away_hbm,
    here_hbm,
    mean_hbm,
    tokens_ref,
    gain_ref,
    go_ref,
    cos_ref,
    sin_ref,
    w_ref,
    nm_ref,
    acc_ref,
    q_ref,
    k_ref,
    v_ref,
    grads_ref,
    shares_ref,
    pieces_ref,
    own_mean_ref,
    all_mean_ref,
    outer_ref,
    in_sems,
    out_sems,
    away_sems,
    here_sems,
    w_sems,
    ag_send,
    ag_recv,
    fr_send,
    fr_recv,
    fg_send,
    fg_recv,
    own_sem,
):
    me = lax.axis_index("tp")
    peer = 1 - me
    rep = lax.axis_index("rep")
    rows, width = tokens_ref.shape
    qw, kw = wq_hbm.shape[1], wk_hbm.shape[1]
    total = qw + 2 * kw
    cw = width // chunks
    piece_rows, piece_cols = own_mean_ref.shape
    col_blocks = width // piece_cols
    loads = [
        pltpu.make_async_copy(source, target, in_sems.at[i])
        for i, (source, target) in enumerate(
            (
                (tokens_hbm, tokens_ref),
                (gain_hbm, gain_ref),
                (cos_hbm, cos_ref),
                (sin_hbm, sin_ref),
                (go_hbm, go_ref),
            )
        )
    ]
    for copy in loads:
        copy.start()
    barrier = pltpu.get_barrier_semaphore()
    pl.semaphore_signal(barrier, inc=1, device_id={"tp": peer}, device_id_type=MESH)

    def greet(j, _):
        pl.semaphore_signal(
            barrier, inc=1, device_id={"rep": lax.rem(rep + j, n_rep)}, device_id_type=MESH
        )
        return 0

    lax.fori_loop(1, n_rep, greet, 0)
    weight_copies = [
        pltpu.make_async_copy(wq_hbm, w_ref.at[:, pl.ds(0, qw)], w_sems.at[0]),
        pltpu.make_async_copy(wk_hbm, w_ref.at[:, pl.ds(qw, kw)], w_sems.at[1]),
        pltpu.make_async_copy(wv_hbm, w_ref.at[:, pl.ds(qw + kw, kw)], w_sems.at[2]),
    ]
    for copy in weight_copies:
        copy.start()

    def piece(owner):
        return (
            ds(owner // col_blocks, piece_rows),
            ds(lax.rem(owner, col_blocks), piece_cols),
        )

    own_piece = pltpu.make_async_copy(local_hbm.at[piece(rep)], pieces_ref.at[0], own_sem.at[0])
    own_piece.start()
    own_outer = pltpu.make_async_copy(outer_hbm.at[piece(rep)], outer_ref, own_sem.at[1])
    own_outer.start()

    for copy in loads:
        copy.wait()
    step = 16

    def norm_rows(i, _):
        x = tokens_ref[ds(i, step), :].astype(jnp.float32)
        inverse = lax.rsqrt(jnp.mean(x * x, axis=-1, keepdims=True) + epsilon)
        nm_ref[pl.ds(pl.multiple_of(me * rows + i * step, step), step), :] = (
            x * inverse * gain_ref[...]
        ).astype(jnp.bfloat16)
        return 0

    lax.fori_loop(0, rows // step, norm_rows, 0)
    pl.semaphore_wait(barrier, n_rep)

    def gather_copy(c):
        part = nm_ref.at[ds(me, rows), ds(c, cw)]
        return pltpu.make_async_remote_copy(
            src_ref=part,
            dst_ref=part,
            send_sem=ag_send.at[c],
            recv_sem=ag_recv.at[c],
            device_id={"tp": peer},
            device_id_type=MESH,
        )

    def scatter_copy(j):
        target = lax.rem(rep + j, n_rep)
        return pltpu.make_async_remote_copy(
            src_ref=local_hbm.at[piece(target)],
            dst_ref=pieces_ref.at[j],
            send_sem=fr_send.at[j],
            recv_sem=fr_recv.at[j],
            device_id={"rep": target},
            device_id_type=MESH,
        )

    def spread_copy(j, owner):
        return pltpu.make_async_remote_copy(
            src_ref=own_mean_ref,
            dst_ref=all_mean_ref.at[piece(owner)],
            send_sem=fg_send.at[j],
            recv_sem=fg_recv.at[j],
            device_id={"rep": lax.rem(rep + j, n_rep)},
            device_id_type=MESH,
        )

    def start_all(make, low, high):
        def one(j, _):
            make(j).start()
            return 0

        lax.fori_loop(low, high, one, 0)

    def wait_recv_all(make, low, high):
        def one(j, _):
            make(j).wait_recv()
            return 0

        lax.fori_loop(low, high, one, 0)

    def wait_send_all(make, low, high):
        def one(j, _):
            make(j).wait_send()
            return 0

        lax.fori_loop(low, high, one, 0)

    start_all(gather_copy, 0, chunks)
    start_all(scatter_copy, 1, n_rep)

    for copy in weight_copies:
        copy.wait()

    def own_tile(t, _):
        acc_ref[ds(me, rows), ds(t, tile)] = dot(nm_ref[ds(me, rows), :], w_ref[:, ds(t, tile)])
        return 0

    lax.fori_loop(0, total // tile, own_tile, 0)
    acc_ref[ds(peer, rows), :] = jnp.zeros((rows, total), jnp.float32)

    own_piece.wait()
    own_outer.wait()
    wait_recv_all(scatter_copy, 1, n_rep)
    summed = pieces_ref[0].astype(jnp.float32)
    for j in range(1, n_rep):
        summed = summed + pieces_ref[j].astype(jnp.float32)
    summed = (outer_ref[...] - summed * (1.0 / n_rep)).astype(jnp.bfloat16)
    own_mean_ref[...] = summed
    all_mean_ref[piece(rep)] = summed
    start_all(lambda j: spread_copy(j, rep), 1, n_rep)

    def arrived(c, _):
        pltpu.make_async_remote_copy(
            src_ref=nm_ref.at[ds(peer, rows), ds(c, cw)],
            dst_ref=nm_ref.at[ds(peer, rows), ds(c, cw)],
            send_sem=ag_send.at[c],
            recv_sem=ag_recv.at[c],
            device_id={"tp": peer},
            device_id_type=MESH,
        ).wait_recv()
        part = nm_ref[ds(peer, rows), ds(c, cw)]

        def one(t, _):
            acc_ref[ds(peer, rows), ds(t, tile)] += dot(part, w_ref[ds(c, cw), ds(t, tile)])
            return 0

        lax.fori_loop(0, total // tile, one, 0)
        return 0

    lax.fori_loop(0, chunks, arrived, 0)

    normed_out = pltpu.make_async_copy(nm_ref, normed_hbm, out_sems.at[0])
    normed_out.start()
    cosine, sine = cos_ref[...], sin_ref[...]

    def rope_head(source, target, index):
        vector = acc_ref[:, ds(source, HEAD_SIZE)]
        target[:, ds(index, HEAD_SIZE)] = (
            vector * cosine + pltpu.roll(vector, HEAD_SIZE // 2, 1) * sine
        ).astype(jnp.bfloat16)

    heads_q, heads_kv = qw // HEAD_SIZE, kw // HEAD_SIZE
    for h in range(heads_q):
        rope_head(h, q_ref, h)
    for h in range(heads_kv):
        rope_head(heads_q + h, k_ref, h)
    v_ref[...] = acc_ref[:, pl.ds(qw + kw, kw)].astype(jnp.bfloat16)

    sequence = 2 * rows
    group = heads_q // heads_kv
    scale = HEAD_SIZE ** (-0.5)

    def reverse(gradient, block):
        c = cosine[block * rows : (block + 1) * rows]
        s = sine[block * rows : (block + 1) * rows]
        return (gradient * c - pltpu.roll(gradient, HEAD_SIZE // 2, 1) * s).astype(jnp.bfloat16)

    def kv_head(g, _):
        grad_k = [None, None]
        grad_v = [None, None]
        for r in range(group):
            head = ds(g * group + r, HEAD_SIZE)
            for b in range(2):
                keys = (b + 1) * rows
                block = pl.ds(b * rows, rows)
                query = q_ref[block, head]
                out_grad = go_ref[block, head]
                key = k_ref[pl.ds(0, keys), ds(g, HEAD_SIZE)]
                value = v_ref[pl.ds(0, keys), ds(g, HEAD_SIZE)]
                scores = dot(query, key, NT) * scale
                row = lax.broadcasted_iota(jnp.int32, scores.shape, 0) + b * rows
                col = lax.broadcasted_iota(jnp.int32, scores.shape, 1)
                scores = jnp.where(col <= row, scores, -jnp.inf)
                powers = jnp.exp(scores - jnp.max(scores, axis=-1, keepdims=True))
                prob = powers * (1.0 / jnp.sum(powers, axis=-1, keepdims=True))
                grad_prob = dot(out_grad, value, NT)
                inner = jnp.sum(grad_prob * prob, axis=-1, keepdims=True)
                score_low = (prob * (grad_prob - inner) * scale).astype(jnp.bfloat16)
                grads_ref[block, head] = reverse(dot(score_low, key), b)
                part_v = dot(prob.astype(jnp.bfloat16), out_grad, TN)
                part_k = dot(score_low, query, TN)
                for j in range(b + 1):
                    pv = part_v[j * rows : (j + 1) * rows]
                    pk = part_k[j * rows : (j + 1) * rows]
                    grad_v[j] = pv if grad_v[j] is None else grad_v[j] + pv
                    grad_k[j] = pk if grad_k[j] is None else grad_k[j] + pk
        for j in range(2):
            block = pl.ds(j * rows, rows)
            grads_ref[block, ds(heads_q + g, HEAD_SIZE)] = reverse(grad_k[j], j)
            grads_ref[block, ds(heads_q + heads_kv + g, HEAD_SIZE)] = grad_v[j].astype(jnp.bfloat16)
        return 0

    lax.fori_loop(0, heads_kv, kv_head, 0)

    grads_out = pltpu.make_async_copy(grads_ref, grads_hbm, out_sems.at[1])
    grads_out.start()

    def away_copy(c):
        columns = ds(c, cw)
        return pltpu.make_async_copy(
            shares_ref.at[ds(peer, rows), columns], away_hbm.at[:, columns], away_sems.at[c]
        )

    def here_copy(c):
        columns = ds(c, cw)
        return pltpu.make_async_copy(
            shares_ref.at[ds(me, rows), columns], here_hbm.at[:, columns], here_sems.at[c]
        )

    def share(c, _):
        shares_ref[:, ds(c, cw)] = dot(grads_ref[...], w_ref[ds(c, cw), :], NT).astype(
            jnp.bfloat16
        )
        away_copy(c).start()
        here_copy(c).start()
        return 0

    lax.fori_loop(0, chunks, share, 0)
    wait_recv_all(lambda j: spread_copy(j, lax.rem(rep + n_rep - j, n_rep)), 1, n_rep)
    mean_out = pltpu.make_async_copy(all_mean_ref, mean_hbm, out_sems.at[2])
    mean_out.start()
    wait_send_all(gather_copy, 0, chunks)
    wait_send_all(scatter_copy, 1, n_rep)
    wait_send_all(lambda j: spread_copy(j, rep), 1, n_rep)
    normed_out.wait()
    grads_out.wait()
    mean_out.wait()
    for c in range(chunks):
        away_copy(c).wait()
        here_copy(c).wait()


def weight_kernel(
    rows,
    normed_ref,
    grads_ref,
    away_ref,
    here_ref,
    gain_ref,
    momentum_ref,
    global_ref,
    mean_ref,
    dwq_ref,
    dwk_ref,
    dwv_ref,
    gain_out,
    new_global,
    new_momentum,
):
    me = lax.axis_index("tp")
    qw, kw = dwq_ref.shape[1], dwk_ref.shape[1]
    own = ds(me, rows)
    columns = ds(pl.program_id(0), normed_ref.shape[1])
    turned = normed_ref[...].T
    dwq_ref[...] = dot(turned, grads_ref[:, pl.ds(0, qw)]).astype(jnp.bfloat16)
    dwk_ref[...] = dot(turned, grads_ref[:, pl.ds(qw, kw)]).astype(jnp.bfloat16)
    dwv_ref[...] = dot(turned, grads_ref[:, pl.ds(qw + kw, kw)]).astype(jnp.bfloat16)
    products = here_ref[...].astype(jnp.float32) * normed_ref[own, :].astype(jnp.float32)
    products += away_ref[...].astype(jnp.float32) * normed_ref[ds(1 - me, rows), :].astype(
        jnp.float32
    )
    gain_out[:, columns] = jnp.sum(products, axis=0, keepdims=True) / gain_ref[...]
    outer = global_ref[...]
    mean_delta = mean_ref[...].astype(jnp.float32)
    updated = outer_momentum * momentum_ref[...] + mean_delta
    new_momentum[...] = updated
    new_global[...] = outer - outer_rate * (mean_delta + outer_momentum * updated)


def tail_kernel(tokens_ref, gain_ref, here_ref, landed_ref, mine_ref, other_ref, out_ref, total_ref):
    x = tokens_ref[...].astype(jnp.float32)
    inverse = lax.rsqrt(jnp.mean(x * x, axis=-1, keepdims=True) + epsilon)
    xhat = x * inverse
    band = tokens_ref.shape[0]
    landed = landed_ref[ds(pl.program_id(0), band), :].astype(jnp.float32)
    here = here_ref[ds(pl.program_id(0), band), :].astype(jnp.float32)
    scaled = (here + landed) * gain_ref[...]
    inner = jnp.mean(scaled * xhat, axis=-1, keepdims=True)
    out_ref[...] = (inverse * (scaled - xhat * inner)).astype(jnp.bfloat16)
    total_ref[...] = mine_ref[...] + other_ref[...]


def pair_body(
    n_rep,
    tokens,
    norm_gain,
    w_query,
    key_weight,
    value_weight,
    attention_gradient,
    global_fragment,
    momentum,
    local_fragment,
):
    rows, width = tokens.shape[1:]
    sequence = 2 * rows
    weight_q, weight_k, weight_v = w_query[0], key_weight[0], value_weight[0]
    qw, kw = weight_q.shape[1], weight_k.shape[1]
    total = qw + 2 * kw
    frag_rows = local_fragment.shape[1]
    piece_rows = 16
    piece_cols = width * frag_rows // piece_rows // n_rep
    chunks = 6
    bf16, f32 = jnp.bfloat16, jnp.float32
    cosine, sine = host_tables(sequence, HEAD_SIZE)
    vmem = pl.BlockSpec(memory_space=pltpu.VMEM)
    anyspace = pl.BlockSpec(memory_space=pl.ANY)
    normed, grads, away, here, mean_delta = pl.pallas_call(
        functools.partial(front_kernel, n_rep, chunks, 512),
        out_shape=(
            jax.ShapeDtypeStruct((sequence, width), bf16),
            jax.ShapeDtypeStruct((sequence, total), bf16),
            jax.ShapeDtypeStruct((rows, width), bf16),
            jax.ShapeDtypeStruct((rows, width), bf16),
            jax.ShapeDtypeStruct((frag_rows, width), bf16),
        ),
        in_specs=[anyspace] * 10,
        out_specs=(anyspace,) * 5,
        scratch_shapes=[
            pltpu.VMEM((rows, width), bf16),
            pltpu.VMEM((1, width), f32),
            pltpu.VMEM((sequence, qw), bf16),
            pltpu.VMEM((sequence, HEAD_SIZE), f32),
            pltpu.VMEM((sequence, HEAD_SIZE), f32),
            pltpu.VMEM((width, total), bf16),
            pltpu.VMEM((sequence, width), bf16),
            pltpu.VMEM((sequence, total), f32),
            pltpu.VMEM((sequence, qw), bf16),
            pltpu.VMEM((sequence, kw), bf16),
            pltpu.VMEM((sequence, kw), bf16),
            pltpu.VMEM((sequence, total), bf16),
            pltpu.VMEM((sequence, width), bf16),
            pltpu.VMEM((n_rep, piece_rows, piece_cols), bf16),
            pltpu.VMEM((piece_rows, piece_cols), bf16),
            pltpu.VMEM((frag_rows, width), bf16),
            pltpu.VMEM((piece_rows, piece_cols), f32),
            pltpu.SemaphoreType.DMA((5,)),
            pltpu.SemaphoreType.DMA((3,)),
            pltpu.SemaphoreType.DMA((chunks,)),
            pltpu.SemaphoreType.DMA((chunks,)),
            pltpu.SemaphoreType.DMA((3,)),
            pltpu.SemaphoreType.DMA((chunks,)),
            pltpu.SemaphoreType.DMA((chunks,)),
            pltpu.SemaphoreType.DMA((n_rep,)),
            pltpu.SemaphoreType.DMA((n_rep,)),
            pltpu.SemaphoreType.DMA((n_rep,)),
            pltpu.SemaphoreType.DMA((n_rep,)),
            pltpu.SemaphoreType.DMA((2,)),
        ],
        compiler_params=pltpu.CompilerParams(
            collective_id=0, has_side_effects=True, vmem_limit_bytes=60 * 1024 * 1024
        ),
    )(
        tokens[0],
        norm_gain,
        weight_q,
        weight_k,
        weight_v,
        attention_gradient[0],
        cosine,
        sine,
        local_fragment[0],
        global_fragment,
    )
    swap = [(0, 1), (1, 0)]
    landed = lax.ppermute(away, "tp", swap)
    cw = width // chunks

    def columns(height):
        return pl.BlockSpec((height, cw), lambda i: (0, i))

    def rows_of(breadth):
        return pl.BlockSpec((cw, breadth), lambda i: (i, 0))

    grad_wq, grad_wk, grad_wv, gain_partial, new_global, new_momentum = pl.pallas_call(
        functools.partial(weight_kernel, rows),
        grid=(chunks,),
        out_shape=(
            jax.ShapeDtypeStruct((width, qw), bf16),
            jax.ShapeDtypeStruct((width, kw), bf16),
            jax.ShapeDtypeStruct((width, kw), bf16),
            jax.ShapeDtypeStruct((1, width), f32),
            jax.ShapeDtypeStruct((frag_rows, width), f32),
            jax.ShapeDtypeStruct((frag_rows, width), f32),
        ),
        in_specs=[
            columns(sequence),
            pl.BlockSpec((sequence, total), lambda i: (0, 0)),
            columns(rows),
            columns(rows),
            columns(1),
            columns(frag_rows),
            columns(frag_rows),
            columns(frag_rows),
        ],
        out_specs=(
            rows_of(qw),
            rows_of(kw),
            rows_of(kw),
            vmem,
            columns(frag_rows),
            columns(frag_rows),
        ),
        compiler_params=pltpu.CompilerParams(vmem_limit_bytes=52 * 1024 * 1024),
        cost_estimate=pl.CostEstimate(
            flops=2 * sequence * width * total,
            bytes_accessed=2 * width * total + 12 * frag_rows * width * 2,
            transcendentals=0,
        ),
    )(
        normed,
        grads,
        away,
        here,
        norm_gain,
        momentum,
        global_fragment,
        mean_delta,
    )
    gain_other = lax.ppermute(gain_partial, "tp", swap)
    band = 32
    row_block = pl.BlockSpec((band, width), lambda i: (i, 0))
    whole_row = pl.BlockSpec((1, width), lambda i: (0, 0))
    gradient_rows, gains_gradient = pl.pallas_call(
        tail_kernel,
        grid=(rows // band,),
        out_shape=(
            jax.ShapeDtypeStruct((rows, width), bf16),
            jax.ShapeDtypeStruct((1, width), f32),
        ),
        in_specs=[row_block, whole_row, vmem, vmem, vmem, vmem],
        out_specs=(row_block, whole_row),
        compiler_params=pltpu.CompilerParams(vmem_limit_bytes=16 * 1024 * 1024),
        cost_estimate=pl.CostEstimate(
            flops=10 * rows * width, bytes_accessed=8 * rows * width, transcendentals=0
        ),
    )(tokens[0], norm_gain, here, landed, gain_partial, gain_other)
    return (
        grad_wq[None],
        grad_wk[None],
        grad_wv[None],
        gains_gradient,
        gradient_rows[None],
        new_global,
        new_momentum,
    )


def solution(mesh):
    placed = (
        P("rep", "tp", None),
        P("rep", None),
        P("rep", None, "tp"),
        P("rep", None, "tp"),
        P("rep", None, "tp"),
        P("rep", None, "tp"),
        P("tp", None),
        P("tp", None),
        P("rep", "tp", None),
    )
    paired = mesh.shape["tp"] == 2
    chosen = functools.partial(pair_body, mesh.shape["rep"]) if paired else body
    return jax.shard_map(
        chosen,
        mesh=mesh,
        in_specs=placed,
        out_specs=(
            P("rep", None, "tp"),
            P("rep", None, "tp"),
            P("rep", None, "tp"),
            P("rep", None),
            P("rep", "tp", None),
            P("tp", None),
            P("tp", None),
        ),
        check_vma=False,
    )
```
